32 devices in a mesh: groups: 2 (over y), ep: 16 (over z, x, core).
Axes of the slice: x: 2, y: 2, z: 4, core: 2. Of those that a mesh axis runs over, the one named last changes fastest.
Arguments:
- tokens: bfloat16 [128, 7168], P(('groups', 'ep')), parts along dimension 0, may hold values from -6 to 6
- routes: int32 [128, 8], P(('groups', 'ep')), parts along dimension 0, may hold values from 0 to 15, as said below
- gates: float32 [128, 8], P(('groups', 'ep')), parts along dimension 0, may hold values from 0.05 to 0.6
- gate_weight: bfloat16 [7168, 32768], P(None, 'ep'), may hold values from -0.0625 to 0.0625
- up_weight: bfloat16 [7168, 32768], P(None, 'ep'), may hold values from -0.0625 to 0.0625
- down_weight: bfloat16 [32768, 7168], P('ep'), may hold values from -0.125 to 0.125
Outputs:
- mixed: bfloat16 [128, 7168], P(('groups', 'ep')), parts along dimension 0
The draws below stay inside these ranges and needn't reach their ends.
There are 2 independent parts, one for each index of `groups`. The reference program is written for one: setup_inputs(seed, part) draws one part's arguments, and reference() takes and returns one part's arrays. A program takes and returns all parts, laid end to end along the dimension named above; an argument that names none is the same for every part. Nothing has to cross between parts.
Inputs may be any that keep to these rules, and one draw needn't show every extreme that they name: `routes`: each token names 8 different experts. Among the 4 tokens of one device no expert is named by more than 3 of them, and in every draw one expert is named by exactly 3 tokens of every device.
All inputs are finite; a program needn't handle non-finite values.
Results may differ from the reference program's by a relative error of at most 0.0085.
Values may be sent and summed in bfloat16 or wider, within the bound.
A program may use at most 128 MiB of HBM per device.

```python
import math
import jax
import jax.numpy as jnp
from jax import lax

D = 7168
FF = 2048
TOP = 8
EXPERTS = 16
TOK_DEV = 4
CAP = 3
TOKENS = 64


def draw_routes(key, part):
    hot_expert = jax.random.randint(jax.random.fold_in(key, 11), (), 0, EXPERTS).astype(jnp.int32)
    blocks = TOKENS // TOK_DEV
    block_keys = jax.random.split(jax.random.fold_in(key, 12), blocks)
    others = (hot_expert + 1 + jnp.arange(EXPERTS - 1, dtype=jnp.int32)) % EXPERTS
    expert_pool = jnp.repeat(others, CAP)

    def one_block(block_key):
        key_pool, key_rows, key_cols = jax.random.split(block_key, 3)
        shuffled = expert_pool[jax.random.permutation(key_pool, expert_pool.shape[0])]
        chosen = jnp.concatenate([jnp.full((CAP,), hot_expert, jnp.int32), shuffled[:TOK_DEV * TOP - CAP]])
        ordered = jnp.sort(chosen)
        route_table = ordered.reshape(TOP, TOK_DEV).T
        route_table = route_table[jax.random.permutation(key_rows, TOK_DEV)]
        scores = jax.random.randint(key_cols, (TOK_DEV, TOP), 0, 1 << 20) * TOP + jnp.arange(TOP, dtype=jnp.int32)[None, :]
        return jnp.take_along_axis(route_table, jnp.argsort(scores, axis=1), axis=1)
    return jax.vmap(one_block)(block_keys).reshape(TOKENS, TOP).astype(jnp.int32)


def level_of(rng, dims, cuts, low, top_value):
    level = 1.0
    for dim, blocks in cuts:
        draws = jax.random.uniform(jax.random.fold_in(jax.random.fold_in(rng, 6), dim), (blocks,), jnp.float32, low / len(cuts), top_value / len(cuts))
        level = level * jnp.repeat(jnp.exp(draws), dims[dim] // blocks).reshape((-1,) + (1,) * (len(dims) - 1 - dim))
    return level


def gaussian(key, dims, deviation, most, cuts=(), kind=jnp.bfloat16):
    gain = level_of(key, dims, cuts, -0.22, 0.18) if cuts else 1.0
    entries = jax.random.normal(key, dims, jnp.float32) * deviation * gain
    return jnp.minimum(jnp.maximum(entries, -most), most).astype(kind)


def setup_inputs(seed: int = 0, part: int = 0) -> dict:
    streams_of = jax.random.split(jax.random.key(seed), 7)
    part_splits = jax.random.split(jax.random.fold_in(streams_of[6], part), 7)
    return {
        "tokens": gaussian(part_splits[0], (TOKENS, D), 1.0, 6.0, ((0, 16),)),
        "routes": draw_routes(jax.random.fold_in(jax.random.fold_in(streams_of[6], part), 71), part),
        "gates": jnp.clip(jnp.exp(math.log(0.6) - 2.4849067 * jax.random.uniform(part_splits[2], (TOKENS, TOP), jnp.float32) ** level_of(part_splits[2], (TOKENS, TOP), ((0, 16),), -0.2, 0.2)), 0.05, 0.6),
        "gate_weight": gaussian(streams_of[3], (D, EXPERTS * FF), D ** -0.5, 0.0625, ((1, 16),)),
        "up_weight": gaussian(streams_of[4], (D, EXPERTS * FF), D ** -0.5, 0.0625, ((1, 16),)),
        "down_weight": gaussian(streams_of[5], (EXPERTS * FF, D), FF ** -0.5, 0.125, ((0, 16),)),
    }


def reference(tokens, routes, gates, gate_weight, up_weight, down_weight):
    bound = CAP * (TOKENS // TOK_DEV)

    def add_expert(running, expert):
        matches = routes == expert
        routed = jnp.any(matches, axis=1)
        weight = jnp.sum(jnp.where(matches, gates, jnp.zeros_like(gates)), axis=1)
        row_order = jnp.argsort(jnp.where(routed, 0, 1).astype(jnp.int32), stable=True)[:bound].astype(jnp.int32)
        picked_rows = tokens[row_order]
        start = (expert * FF).astype(jnp.int32)
        gate_cols = lax.dynamic_slice_in_dim(gate_weight, start, FF, 1)
        up_cols = lax.dynamic_slice_in_dim(up_weight, start, FF, 1)
        down_rows = lax.dynamic_slice_in_dim(down_weight, start, FF, 0)
        gate_act = jnp.dot(picked_rows, gate_cols, preferred_element_type=jnp.float32)
        up_act = jnp.dot(picked_rows, up_cols, preferred_element_type=jnp.float32)
        hidden = (jax.nn.silu(gate_act) * up_act).astype(jnp.bfloat16)
        expert_out = jnp.dot(hidden, down_rows, preferred_element_type=jnp.float32)
        running = running.at[row_order].add(weight[row_order][:, None] * expert_out)
        return running, None

    initial = jnp.zeros(tokens.shape, jnp.float32)
    running, unused = lax.scan(add_expert, initial, jnp.arange(EXPERTS, dtype=jnp.int32))
    return running.astype(jnp.bfloat16)
```

```python
import functools

import jax
import jax.numpy as jnp
from jax import lax
from jax.experimental import pallas as pl
from jax.experimental.pallas import tpu as pltpu
from jax.sharding import PartitionSpec as P

EXPERTS = 16
SLOTS = 7
AHEAD = 2
AUX = 128


def piece(total, want):
    size = want
    while total % size:
        size //= 2
    return size


def split_chips(chips):
    inner = 1
    while inner * inner * 4 <= chips:
        inner *= 2
    return inner


def column_spans(width, big, small):
    spans, at = [], 0
    while at + big < width:
        spans.append((at, big))
        at += big
    for size in (big // 2, small, small):
        size = min(size, width - at)
        if size:
            spans.append((at, size))
            at += size
    return spans


def kernel(
    devices, inner, kc, spans, tile,
    tokens, routes, gates, wg, wu, wd, out,
    ring_g, ring_u, down, rx, ax, xb, acc_g, acc_u, hid, share, mine, theirs, own, xs, xr, zs, zr,
    tok_sem, g_sem, u_sem, d_sem,
    tz_send, tz_recv, tx_send, tx_recv, re_send, re_recv,
    ob_send, ob_recv, rx_send, rx_recv, rz_send, rz_recv, ax_send, ax_recv,
):
    rows, width = tokens.shape
    hidden = wg.shape[1]
    chips = devices // 2
    outer = chips // inner
    block = outer * rows
    slots = ring_g.shape[0]
    units, outs = width // kc, len(spans)
    me = lax.axis_index("ep")
    chip, core = me // 2, me % 2
    z, x = chip // inner, chip % inner
    other = 1 - core
    peer = chip * 2 + other
    line = (core * inner + x) * outer
    mates = chips * rows

    def place(to_z, to_x):
        return (to_z * inner + to_x) * 2 + core

    def along_z(i):
        return lax.rem(z + i, outer)

    def along_x(i):
        return lax.rem(x + i, inner)

    def remote(src, dst, send, recv, dev):
        return pltpu.make_async_remote_copy(
            src_ref=src, dst_ref=dst, send_sem=send, recv_sem=recv,
            device_id={"ep": dev}, device_id_type=pl.DeviceIdType.MESH,
        )

    def many(ref, sem):
        return pltpu.make_async_copy(ref, ref, sem)

    def load_tokens(j):
        return pltpu.make_async_copy(
            tokens.at[:, pl.ds(j * kc, kc)], rx.at[j, line + z], tok_sem.at[j]
        )

    def load_g(j):
        s = j % slots
        return pltpu.make_async_copy(wg.at[pl.ds(j * kc, kc), :], ring_g.at[s], g_sem.at[s])

    def load_u(j):
        s = j % slots
        return pltpu.make_async_copy(wu.at[pl.ds(j * kc, kc), :], ring_u.at[s], u_sem.at[s])

    def load_d(c):
        cols = pl.ds(*spans[c])
        return pltpu.make_async_copy(wd.at[:, cols], down.at[:, cols], d_sem.at[c])

    for j in range(units):
        load_tokens(j).start()
    for j in range(min(slots, units)):
        load_g(j).start()
        load_u(j).start()
    issued = min(AHEAD, outs)
    for c in range(issued):
        load_d(c).start(priority=1)

    barrier = pltpu.get_barrier_semaphore()

    def greet(dev):
        pl.semaphore_signal(barrier, inc=1, device_id={"ep": dev}, device_id_type=pl.DeviceIdType.MESH)

    for i in range(1, outer):
        greet(place(along_z(i), x))
    for i in range(1, inner):
        greet(place(z, along_x(i)))
    greet(peer)

    lane = lax.broadcasted_iota(jnp.int32, (rows, AUX), 1)
    name = jnp.where(lane < EXPERTS, lane, lane - EXPERTS)
    weight = jnp.zeros((rows, AUX), jnp.float32)
    for k in range(routes.shape[1]):
        weight = weight + jnp.where(routes[:, k : k + 1] == name, gates[:, k : k + 1], 0.0)
    high = weight.astype(jnp.bfloat16).astype(jnp.float32)
    ax[line + z] = jnp.where(
        lane < EXPERTS, high, jnp.where(lane < 2 * EXPERTS, weight - high, 0.0)
    ).astype(jnp.bfloat16)

    pl.semaphore_wait(barrier, outer + inner - 1)

    for j in range(units):
        load_tokens(j).wait()
        for i in range(1, outer):
            slot = rx.at[j, line + z]
            remote(slot, slot, tz_send.at[j], tz_recv.at[j], place(along_z(i), x)).start()
    for i in range(1, outer):
        slot = ax.at[line + z]
        remote(slot, slot, ax_send.at[0], ax_recv.at[0], place(along_z(i), x)).start()

    def hop_x(j):
        many(rx.at[j, pl.ds(0, outer - 1)], tz_recv.at[j]).wait()
        for i in range(1, inner):
            part = rx.at[j, pl.ds(line, outer)]
            remote(part, part, tx_send.at[j], tx_recv.at[j], place(z, along_x(i))).start()

    def relay(j):
        half = rx.at[j, pl.ds(core * chips, chips)]
        return remote(half, half, re_send.at[j], re_recv.at[j], peer)

    def hop_core(j):
        many(rx.at[j, pl.ds(0, chips - outer)], tx_recv.at[j]).wait()
        relay(j).start()

    half_ax = ax.at[pl.ds(core * chips, chips)]
    relay_aux = remote(half_ax, half_ax, ax_send.at[2], ax_recv.at[2], peer)

    lead = min(units, LEAD)
    ahead = min(units, LEAD2)
    for j in range(lead):
        hop_x(j)
    sent = 0
    for j in range(lead, units):
        hop_x(j)
        if sent < ahead:
            hop_core(sent)
            sent += 1
    many(ax.at[pl.ds(0, outer - 1)], ax_recv.at[0]).wait()
    for i in range(1, inner):
        part = ax.at[pl.ds(line, outer)]
        remote(part, part, ax_send.at[1], ax_recv.at[1], place(z, along_x(i))).start()

    group = max(1, 16 // rows)

    def gather_rows(j, b):
        parts = [rx[j, b * group + i].astype(jnp.float32) for i in range(group)]
        whole = parts[0] if group == 1 else jnp.concatenate(parts, axis=0)
        return whole.astype(jnp.bfloat16)

    for j in range(units):
        while sent < min(units, j + 1 + ahead):
            hop_core(sent)
            sent += 1
        relay(j).wait_recv()
        if devices // group <= 16:
            for b in range(devices // group):
                xb[b * group * rows : (b + 1) * group * rows, :] = gather_rows(j, b)
        else:
            @pl.loop(0, devices // group)
            def _(b):
                xb[pl.ds(pl.multiple_of(b * group * rows, group * rows), group * rows), :] = gather_rows(j, b)
        load_g(j).wait()
        load_u(j).wait()
        s = j % slots

        for n in range(hidden // tile):
            cols = pl.ds(n * tile, tile)
            pg = jnp.dot(xb[...], ring_g[s, :, cols], preferred_element_type=jnp.float32)
            pu = jnp.dot(xb[...], ring_u[s, :, cols], preferred_element_type=jnp.float32)
            if j == 0:
                acc_g[:, cols] = pg
                acc_u[:, cols] = pu
            elif j < units - 1:
                acc_g[:, cols] += pg
                acc_u[:, cols] += pu
            else:
                g = acc_g[:, cols] + pg
                u = acc_u[:, cols] + pu
                hid[:, cols] = (g / (1.0 + jnp.exp(-g)) * u).astype(jnp.bfloat16)

        if j + slots < units:
            load_g(j + slots).start()
            load_u(j + slots).start()
        if j + slots + 1 >= units:
            while issued < outs:
                load_d(issued).start(priority=1)
                issued += 1

    many(ax.at[pl.ds(0, chips - outer)], ax_recv.at[1]).wait()
    relay_aux.start()
    relay_aux.wait_recv()
    expert = me // (devices // EXPERTS)
    spot = lax.broadcasted_iota(jnp.int32, (group * rows, AUX), 1)
    hot = (spot == expert) | (spot == expert + EXPERTS)

    def share_rows(b):
        parts = [ax[b * group + i].astype(jnp.float32) for i in range(group)]
        whole = parts[0] if group == 1 else jnp.concatenate(parts, axis=0)
        total = jnp.sum(jnp.where(hot, whole, 0.0), axis=1, keepdims=True)
        return jnp.broadcast_to(total, (group * rows, AUX))

    if devices // group <= 16:
        for b in range(devices // group):
            share[b * group * rows : (b + 1) * group * rows, :] = share_rows(b)
    else:
        @pl.loop(0, devices // group)
        def _(b):
            share[pl.ds(pl.multiple_of(b * group * rows, group * rows), group * rows), :] = share_rows(b)

    def swap(c):
        cols = pl.ds(*spans[c])
        return remote(mine.at[other, :, cols], theirs.at[:, cols], ob_send.at[c], ob_recv.at[c], peer)

    def sum_core(c):
        cols = pl.ds(*spans[c])
        swap(c).wait_recv()
        for i in range(1, inner):
            to = along_x(i)
            at = pl.ds(pl.multiple_of(to * block, block), block)
            xs[to, :, cols] = (mine[core, at, cols] + theirs[at, cols]).astype(jnp.bfloat16)
            remote(
                xs.at[to, :, cols], xr.at[x, :, cols], rx_send.at[c], rx_recv.at[c], place(z, to)
            ).start()
        at = pl.ds(pl.multiple_of(x * block, block), block)
        own[:, cols] = mine[core, at, cols] + theirs[at, cols]

    def sum_x(c):
        cols = pl.ds(*spans[c])
        many(xr.at[pl.ds(0, inner - 1), :, cols], rx_recv.at[c]).wait()
        total = own[:, cols]
        for i in range(1, inner):
            total = total + xr[along_x(i), :, cols].astype(jnp.float32)
        for b in range(outer):
            zs[b, :, cols] = total[b * rows : (b + 1) * rows].astype(jnp.bfloat16)
        for i in range(1, outer):
            to = along_z(i)
            remote(
                zs.at[to, :, cols], zr.at[z, :, cols], rz_send.at[c], rz_recv.at[c], place(to, x)
            ).start()
        zr[z, :, cols] = zs[z, :, cols]

    def sum_z(c):
        cols = pl.ds(*spans[c])
        many(zr.at[pl.ds(0, outer - 1), :, cols], rz_recv.at[c]).wait()
        total = zr[0, :, cols].astype(jnp.float32)
        for b in range(1, outer):
            total = total + zr[b, :, cols].astype(jnp.float32)
        out[:, cols] = total.astype(jnp.bfloat16)

    stages = ((LAGS[0], sum_core), (LAGS[1], sum_x), (LAGS[2], sum_z))
    for c in range(outs + LAGS[2]):
        if c < outs:
            load_d(c).wait()
            at, size = spans[c]
            sub = min(tile, size)
            for n in range(size // sub):
                cols = pl.ds(at + n * sub, sub)
                o = jnp.dot(hid[...], down[:, cols], preferred_element_type=jnp.float32)
                o = o * share[:, :1]
                mine[0, :, cols] = o[:mates]
                mine[1, :, cols] = o[mates:]
            swap(c).start()
        for lag, stage in stages:
            if 0 <= c - lag < outs:
                stage(c - lag)

    for j in range(units):
        many(rx.at[j, pl.ds(0, outer - 1)], tz_send.at[j]).wait()
        many(rx.at[j, pl.ds(0, chips - outer)], tx_send.at[j]).wait()
        relay(j).wait_send()
    many(ax.at[pl.ds(0, outer - 1)], ax_send.at[0]).wait()
    many(ax.at[pl.ds(0, chips - outer)], ax_send.at[1]).wait()
    relay_aux.wait_send()
    for c in range(outs):
        cols = pl.ds(*spans[c])
        swap(c).wait_send()
        many(xr.at[pl.ds(0, inner - 1), :, cols], rx_send.at[c]).wait()
        many(zr.at[pl.ds(0, outer - 1), :, cols], rz_send.at[c]).wait()


LEAD, LEAD2 = 4, 3
LAGS = (1, 3, 6)


def layer(tokens, routes, gates, wg, wu, wd):
    devices = lax.axis_size("ep")
    rows, width = tokens.shape
    hidden = wg.shape[1]
    chips = devices // 2
    inner = split_chips(chips)
    outer = chips // inner
    kc = piece(width, 512)
    tile = piece(hidden, 512)
    spans = column_spans(width, piece(width, 1024), 256)
    units, outs = width // kc, len(spans)
    slots = min(SLOTS, units)
    batch = devices * rows
    bf16, f32 = jnp.bfloat16, jnp.float32
    dma = pltpu.SemaphoreType.DMA
    anywhere = pl.BlockSpec(memory_space=pl.ANY)
    vmem = pl.BlockSpec(memory_space=pltpu.VMEM)
    return pl.pallas_call(
        functools.partial(kernel, devices, inner, kc, spans, tile),
        out_shape=pltpu.VMEM((rows, width), bf16),
        in_specs=[anywhere, vmem, vmem, anywhere, anywhere, anywhere],
        out_specs=vmem,
        scratch_shapes=[
            pltpu.VMEM((slots, kc, hidden), bf16),
            pltpu.VMEM((slots, kc, hidden), bf16),
            pltpu.VMEM((hidden, width), bf16),
            pltpu.VMEM((units, devices, rows, kc), bf16),
            pltpu.VMEM((devices, rows, AUX), bf16),
            pltpu.VMEM((batch, kc), bf16),
            pltpu.VMEM((batch, hidden), f32),
            pltpu.VMEM((batch, hidden), f32),
            pltpu.VMEM((batch, hidden), bf16),
            pltpu.VMEM((batch, AUX), f32),
            pltpu.VMEM((2, chips * rows, width), f32),
            pltpu.VMEM((chips * rows, width), f32),
            pltpu.VMEM((outer * rows, width), f32),
            pltpu.VMEM((inner, outer * rows, width), bf16),
            pltpu.VMEM((inner, outer * rows, width), bf16),
            pltpu.VMEM((outer, rows, width), bf16),
            pltpu.VMEM((outer, rows, width), bf16),
            dma((units,)), dma((slots,)), dma((slots,)), dma((outs,)),
            dma((units,)), dma((units,)), dma((units,)), dma((units,)), dma((units,)), dma((units,)),
            dma((outs,)), dma((outs,)), dma((outs,)), dma((outs,)), dma((outs,)), dma((outs,)),
            dma((3,)), dma((3,)),
        ],
        compiler_params=pltpu.CompilerParams(
            collective_id=0, has_side_effects=True, vmem_limit_bytes=66_800_000
        ),
    )(tokens, routes, gates, wg, wu, wd)


def solution(mesh):
    placed = (
        P(("groups", "ep"), None),
        P(("groups", "ep"), None),
        P(("groups", "ep"), None),
        P(None, "ep"),
        P(None, "ep"),
        P("ep", None),
    )
    return jax.shard_map(
        layer, mesh=mesh, in_specs=placed, out_specs=P(("groups", "ep"), None), check_vma=False
    )
```

```python
import functools

import jax
import jax.numpy as jnp
from jax import lax
from jax.experimental import pallas as pl
from jax.experimental.pallas import tpu as pltpu
from jax.sharding import PartitionSpec as P

EXPERTS = 16
SLOTS = 7
AHEAD = 1
WINDOW = 5
LEAD, LEAD2 = 4, 3
LAGS = (1, 4, 8)
TAIL = [512, 256, 256]
DIRECT = 1
AUX = 128


def piece(total, want):
    size = want
    while total % size:
        size //= 2
    return size


def split_chips(chips):
    inner = 1
    while inner * inner * 4 <= chips:
        inner *= 2
    return inner


def column_spans(width, big):
    sizes, left = [], width - sum(TAIL)
    while left:
        sizes.append(min(big, left))
        left -= sizes[-1]
    sizes += TAIL
    return [(sum(sizes[:i]), size) for i, size in enumerate(sizes)]


def kernel(
    devices, inner, kc, spans, tile,
    tokens, routes, gates, wg, wu, wd, out,
    ring_g, ring_u, down, rx, ax, xb, acc_g, acc_u, hid, share, mine, theirs, own, xs, xr, zs, zr, ds, dr,
    tok_sem, g_sem, u_sem, d_sem,
    tz_send, tz_recv, tx_send, tx_recv, re_send, re_recv,
    ob_send, ob_recv, rx_send, rx_recv, rz_send, rz_recv, ax_send, ax_recv,
):
    rows, width = tokens.shape
    hidden = wg.shape[1]
    chips = devices // 2
    outer = chips // inner
    block = outer * rows
    slots = ring_g.shape[0]
    units, outs = width // kc, len(spans)
    me = lax.axis_index("ep")
    chip, core = me // 2, me % 2
    z, x = chip // inner, chip % inner
    other = 1 - core
    peer = chip * 2 + other
    line = (core * inner + x) * outer
    mates = chips * rows

    def place(to_z, to_x):
        return (to_z * inner + to_x) * 2 + core

    def along_z(i):
        return lax.rem(z + i, outer)

    def along_x(i):
        return lax.rem(x + i, inner)

    def remote(src, dst, send, recv, dev):
        return pltpu.make_async_remote_copy(
            src_ref=src, dst_ref=dst, send_sem=send, recv_sem=recv,
            device_id={"ep": dev}, device_id_type=pl.DeviceIdType.MESH,
        )

    def many(ref, sem):
        return pltpu.make_async_copy(ref, ref, sem)

    def load_tokens(j):
        return pltpu.make_async_copy(
            tokens.at[:, pl.ds(j * kc, kc)], rx.at[j, line + z], tok_sem.at[j]
        )

    def load_g(j):
        s = j % slots
        return pltpu.make_async_copy(wg.at[pl.ds(j * kc, kc), :], ring_g.at[s], g_sem.at[s])

    def load_u(j):
        s = j % slots
        return pltpu.make_async_copy(wu.at[pl.ds(j * kc, kc), :], ring_u.at[s], u_sem.at[s])

    def load_d(c):
        cols = pl.ds(*spans[c])
        return pltpu.make_async_copy(wd.at[:, cols], down.at[:, cols], d_sem.at[c])

    for j in range(units):
        load_tokens(j).start()
    for j in range(min(slots, units)):
        load_g(j).start(priority=1)
        load_u(j).start(priority=1)

    barrier = pltpu.get_barrier_semaphore()

    def greet(dev):
        pl.semaphore_signal(barrier, inc=1, device_id={"ep": dev}, device_id_type=pl.DeviceIdType.MESH)

    for i in range(1, chips):
        greet(lax.rem(chip + i, chips) * 2 + core)
    greet(peer)

    lane = lax.broadcasted_iota(jnp.int32, (rows, AUX), 1)
    name = jnp.where(lane < EXPERTS, lane, lane - EXPERTS)
    weight = jnp.zeros((rows, AUX), jnp.float32)
    for k in range(routes.shape[1]):
        weight = weight + jnp.where(routes[:, k : k + 1] == name, gates[:, k : k + 1], 0.0)
    high = weight.astype(jnp.bfloat16).astype(jnp.float32)
    ax[line + z] = jnp.where(
        lane < EXPERTS, high, jnp.where(lane < 2 * EXPERTS, weight - high, 0.0)
    ).astype(jnp.bfloat16)

    pl.semaphore_wait(barrier, chips)

    for j in range(units):
        load_tokens(j).wait()
        for i in range(1, outer):
            slot = rx.at[j, line + z]
            remote(slot, slot, tz_send.at[j], tz_recv.at[j], place(along_z(i), x)).start()
    for i in range(1, outer):
        slot = ax.at[line + z]
        remote(slot, slot, ax_send.at[0], ax_recv.at[0], place(along_z(i), x)).start()

    def hop_x(j):
        many(rx.at[j, pl.ds(0, outer - 1)], tz_recv.at[j]).wait()
        for i in range(1, inner):
            part = rx.at[j, pl.ds(line, outer)]
            remote(part, part, tx_send.at[j], tx_recv.at[j], place(z, along_x(i))).start()

    def relay(j):
        half = rx.at[j, pl.ds(core * chips, chips)]
        return remote(half, half, re_send.at[j], re_recv.at[j], peer)

    def hop_core(j):
        many(rx.at[j, pl.ds(0, chips - outer)], tx_recv.at[j]).wait()
        relay(j).start()

    half_ax = ax.at[pl.ds(core * chips, chips)]
    relay_aux = remote(half_ax, half_ax, ax_send.at[2], ax_recv.at[2], peer)

    lead = min(units, LEAD)
    ahead = min(units, LEAD2)
    for j in range(lead):
        hop_x(j)
    sent = 0
    for j in range(lead, units):
        hop_x(j)
        if sent < ahead:
            hop_core(sent)
            sent += 1
    many(ax.at[pl.ds(0, outer - 1)], ax_recv.at[0]).wait()
    for i in range(1, inner):
        part = ax.at[pl.ds(line, outer)]
        remote(part, part, ax_send.at[1], ax_recv.at[1], place(z, along_x(i))).start()

    group = max(1, 16 // rows)

    def gather_rows(j, b):
        parts = [rx[j, b * group + i].astype(jnp.float32) for i in range(group)]
        whole = parts[0] if group == 1 else jnp.concatenate(parts, axis=0)
        return whole.astype(jnp.bfloat16)

    issued, waited = 0, 0

    def feed(others, least=0):
        nonlocal issued
        while issued < outs and (
            issued < least
            or others + hidden * sum(n for _, n in spans[waited : issued + 1]) <= WINDOW * 2 * kc * hidden
        ):
            load_d(issued).start(priority=1)
            issued += 1

    feed(units * 2 * kc * hidden, AHEAD)
    for j in range(units):
        while sent < min(units, j + 1 + ahead):
            hop_core(sent)
            sent += 1
        relay(j).wait_recv()
        if devices // group <= 16:
            for b in range(devices // group):
                xb[b * group * rows : (b + 1) * group * rows, :] = gather_rows(j, b)
        else:
            @pl.loop(0, devices // group)
            def _(b):
                xb[pl.ds(pl.multiple_of(b * group * rows, group * rows), group * rows), :] = gather_rows(j, b)
        load_g(j).wait()
        load_u(j).wait()
        s = j % slots

        for n in range(hidden // tile):
            cols = pl.ds(n * tile, tile)
            pg = jnp.dot(xb[...], ring_g[s, :, cols], preferred_element_type=jnp.float32)
            pu = jnp.dot(xb[...], ring_u[s, :, cols], preferred_element_type=jnp.float32)
            if j == 0:
                acc_g[:, cols] = pg
                acc_u[:, cols] = pu
            elif j < units - 1:
                acc_g[:, cols] += pg
                acc_u[:, cols] += pu
            else:
                g = acc_g[:, cols] + pg
                u = acc_u[:, cols] + pu
                hid[:, cols] = (g / (1.0 + jnp.exp(-g)) * u).astype(jnp.bfloat16)

        if j + slots < units:
            load_g(j + slots).start(priority=1)
            load_u(j + slots).start(priority=1)
        feed(kc * 2 * hidden * max(0, min(units, j + 1 + slots) - j - 1))

    many(ax.at[pl.ds(0, chips - outer)], ax_recv.at[1]).wait()
    relay_aux.start()
    relay_aux.wait_recv()
    expert = me // (devices // EXPERTS)
    spot = lax.broadcasted_iota(jnp.int32, (group * rows, AUX), 1)
    hot = (spot == expert) | (spot == expert + EXPERTS)

    def share_rows(b):
        parts = [ax[b * group + i].astype(jnp.float32) for i in range(group)]
        whole = parts[0] if group == 1 else jnp.concatenate(parts, axis=0)
        total = jnp.sum(jnp.where(hot, whole, 0.0), axis=1, keepdims=True)
        return jnp.broadcast_to(total, (group * rows, AUX))

    if devices // group <= 16:
        for b in range(devices // group):
            share[b * group * rows : (b + 1) * group * rows, :] = share_rows(b)
    else:
        @pl.loop(0, devices // group)
        def _(b):
            share[pl.ds(pl.multiple_of(b * group * rows, group * rows), group * rows), :] = share_rows(b)

    def swap(c):
        cols = pl.ds(*spans[c])
        return remote(mine.at[other, :, cols], theirs.at[:, cols], ob_send.at[c], ob_recv.at[c], peer)

    def sum_core(c):
        cols = pl.ds(*spans[c])
        swap(c).wait_recv()
        for i in range(1, inner):
            to = along_x(i)
            at = pl.ds(pl.multiple_of(to * block, block), block)
            xs[to, :, cols] = (mine[core, at, cols] + theirs[at, cols]).astype(jnp.bfloat16)
            remote(
                xs.at[to, :, cols], xr.at[x, :, cols], rx_send.at[c], rx_recv.at[c], place(z, to)
            ).start()
        at = pl.ds(pl.multiple_of(x * block, block), block)
        own[:, cols] = mine[core, at, cols] + theirs[at, cols]

    def sum_x(c):
        cols = pl.ds(*spans[c])
        many(xr.at[pl.ds(0, inner - 1), :, cols], rx_recv.at[c]).wait()
        total = own[:, cols]
        for i in range(1, inner):
            total = total + xr[along_x(i), :, cols].astype(jnp.float32)
        for b in range(outer):
            zs[b, :, cols] = total[b * rows : (b + 1) * rows].astype(jnp.bfloat16)
        for i in range(1, outer):
            to = along_z(i)
            remote(
                zs.at[to, :, cols], zr.at[z, :, cols], rz_send.at[c], rz_recv.at[c], place(to, x)
            ).start()
        zr[z, :, cols] = zs[z, :, cols]

    def sum_z(c):
        cols = pl.ds(*spans[c])
        many(zr.at[pl.ds(0, outer - 1), :, cols], rz_recv.at[c]).wait()
        total = zr[0, :, cols].astype(jnp.float32)
        for b in range(1, outer):
            total = total + zr[b, :, cols].astype(jnp.float32)
        out[:, cols] = total.astype(jnp.bfloat16)

    near = spans[outs - DIRECT][0]

    def give(c):
        at, size = spans[c]
        cols, mine_at = pl.ds(at, size), pl.ds(at - near, size)
        swap(c).wait_recv()
        both = mine[core, :, cols] + theirs[:, cols]
        for b in range(chips):
            ds[b % outer * inner + b // outer, :, mine_at] = both[b * rows : (b + 1) * rows].astype(jnp.bfloat16)
        for i in range(1, chips):
            to = lax.rem(chip + i, chips)
            remote(
                ds.at[to, :, mine_at], dr.at[chip, :, mine_at], rz_send.at[c], rz_recv.at[c], to * 2 + core
            ).start()
        dr[chip, :, mine_at] = ds[chip, :, mine_at]

    def sum_all(c):
        at, size = spans[c]
        cols, mine_at = pl.ds(at, size), pl.ds(at - near, size)
        many(dr.at[pl.ds(0, chips - 1), :, mine_at], rz_recv.at[c]).wait()
        total = dr[0, :, mine_at].astype(jnp.float32)
        for b in range(1, chips):
            total = total + dr[b, :, mine_at].astype(jnp.float32)
        out[:, cols] = total.astype(jnp.bfloat16)

    def stage_1(c):
        if c < outs - DIRECT:
            sum_core(c)
        else:
            give(c)

    def stage_2(c):
        if c < outs - DIRECT:
            sum_x(c)

    def stage_3(c):
        if c < outs - DIRECT:
            sum_z(c)
        else:
            sum_all(c)

    stages = ((LAGS[0], stage_1), (LAGS[1], stage_2), (LAGS[2], stage_3))
    for c in range(outs + LAGS[2]):
        if c < outs:
            load_d(c).wait()
            waited += 1
            feed(0)
            at, size = spans[c]
            sub = min(tile, size)
            for n in range(size // sub):
                cols = pl.ds(at + n * sub, sub)
                o = jnp.dot(hid[...], down[:, cols], preferred_element_type=jnp.float32)
                o = o * share[:, :1]
                mine[0, :, cols] = o[:mates]
                mine[1, :, cols] = o[mates:]
            swap(c).start()
        for lag, stage in stages:
            if 0 <= c - lag < outs:
                stage(c - lag)

    for j in range(units):
        many(rx.at[j, pl.ds(0, outer - 1)], tz_send.at[j]).wait()
        many(rx.at[j, pl.ds(0, chips - outer)], tx_send.at[j]).wait()
        relay(j).wait_send()
    many(ax.at[pl.ds(0, outer - 1)], ax_send.at[0]).wait()
    many(ax.at[pl.ds(0, chips - outer)], ax_send.at[1]).wait()
    relay_aux.wait_send()
    for c in range(outs):
        cols = pl.ds(*spans[c])
        swap(c).wait_send()
        if c < outs - DIRECT:
            many(xr.at[pl.ds(0, inner - 1), :, cols], rx_send.at[c]).wait()
            many(zr.at[pl.ds(0, outer - 1), :, cols], rz_send.at[c]).wait()
        else:
            cols = pl.ds(spans[c][0] - near, spans[c][1])
            many(dr.at[pl.ds(0, chips - 1), :, cols], rz_send.at[c]).wait()


def layer(tokens, routes, gates, wg, wu, wd):
    devices = lax.axis_size("ep")
    rows, width = tokens.shape
    hidden = wg.shape[1]
    chips = devices // 2
    inner = split_chips(chips)
    outer = chips // inner
    kc = piece(width, 512)
    tile = piece(hidden, 512)
    spans = column_spans(width, 1024)
    near = spans[len(spans) - DIRECT][0]
    units, outs = width // kc, len(spans)
    slots = min(SLOTS, units)
    batch = devices * rows
    bf16, f32 = jnp.bfloat16, jnp.float32
    dma = pltpu.SemaphoreType.DMA
    anywhere = pl.BlockSpec(memory_space=pl.ANY)
    vmem = pl.BlockSpec(memory_space=pltpu.VMEM)
    return pl.pallas_call(
        functools.partial(kernel, devices, inner, kc, spans, tile),
        out_shape=pltpu.VMEM((rows, width), bf16),
        in_specs=[anywhere, vmem, vmem, anywhere, anywhere, anywhere],
        out_specs=vmem,
        scratch_shapes=[
            pltpu.VMEM((slots, kc, hidden), bf16),
            pltpu.VMEM((slots, kc, hidden), bf16),
            pltpu.VMEM((hidden, width), bf16),
            pltpu.VMEM((units, devices, rows, kc), bf16),
            pltpu.VMEM((devices, rows, AUX), bf16),
            pltpu.VMEM((batch, kc), bf16),
            pltpu.VMEM((batch, hidden), f32),
            pltpu.VMEM((batch, hidden), f32),
            pltpu.VMEM((batch, hidden), bf16),
            pltpu.VMEM((batch, AUX), f32),
            pltpu.VMEM((2, chips * rows, width), f32),
            pltpu.VMEM((chips * rows, width), f32),
            pltpu.VMEM((outer * rows, near), f32),
            pltpu.VMEM((inner, outer * rows, near), bf16),
            pltpu.VMEM((inner, outer * rows, near), bf16),
            pltpu.VMEM((outer, rows, near), bf16),
            pltpu.VMEM((outer, rows, near), bf16),
            pltpu.VMEM((chips, rows, width - near), bf16),
            pltpu.VMEM((chips, rows, width - near), bf16),
            dma((units,)), dma((slots,)), dma((slots,)), dma((outs,)),
            dma((units,)), dma((units,)), dma((units,)), dma((units,)), dma((units,)), dma((units,)),
            dma((outs,)), dma((outs,)), dma((outs,)), dma((outs,)), dma((outs,)), dma((outs,)),
            dma((3,)), dma((3,)),
        ],
        compiler_params=pltpu.CompilerParams(
            collective_id=0, has_side_effects=True, vmem_limit_bytes=66_800_000
        ),
    )(tokens, routes, gates, wg, wu, wd)


def solution(mesh):
    placed = (
        P(("groups", "ep"), None),
        P(("groups", "ep"), None),
        P(("groups", "ep"), None),
        P(None, "ep"),
        P(None, "ep"),
        P("ep", None),
    )
    return jax.shard_map(
        layer, mesh=mesh, in_specs=placed, out_specs=P(("groups", "ep"), None), check_vma=False
    )
```

```python
import functools

import jax
import jax.numpy as jnp
from jax import lax
from jax.experimental import pallas as pl
from jax.experimental.pallas import tpu as pltpu
from jax.sharding import PartitionSpec as P

EXPERTS = 16
SLOTS = 7
AHEAD = 1
WINDOW = 5
LEAD, LEAD2 = 4, 3
LAGS = (1, 4, 10)
TAIL = [512, 512, 256, 256]
DIRECT = 3
AUX = 128


def piece(total, want):
    size = want
    while total % size:
        size //= 2
    return size


def split_chips(chips):
    inner = 1
    while inner * inner * 4 <= chips:
        inner *= 2
    return inner


def column_spans(width, big):
    sizes, left = [], width - sum(TAIL)
    while left:
        sizes.append(min(big, left))
        left -= sizes[-1]
    sizes += TAIL
    return [(sum(sizes[:i]), size) for i, size in enumerate(sizes)]


def kernel(
    devices, inner, kc, spans, tile,
    tokens, routes, gates, wg, wu, wd, out,
    ring_g, ring_u, down, rx, ax, xb, acc_g, acc_u, hid, share, mine, theirs, own, xs, xr, zs, zr, ds, dr,
    tok_sem, g_sem, u_sem, d_sem,
    tz_send, tz_recv, tx_send, tx_recv, re_send, re_recv,
    ob_send, ob_recv, rx_send, rx_recv, rz_send, rz_recv, ax_send, ax_recv,
):
    rows, width = tokens.shape
    hidden = wg.shape[1]
    chips = devices // 2
    outer = chips // inner
    block = outer * rows
    slots = ring_g.shape[0]
    units, outs = width // kc, len(spans)
    me = lax.axis_index("ep")
    chip, core = me // 2, me % 2
    z, x = chip // inner, chip % inner
    other = 1 - core
    peer = chip * 2 + other
    line = (core * inner + x) * outer
    mates = chips * rows

    def place(to_z, to_x):
        return (to_z * inner + to_x) * 2 + core

    def along_z(i):
        return lax.rem(z + i, outer)

    def along_x(i):
        return lax.rem(x + i, inner)

    def remote(src, dst, send, recv, dev):
        return pltpu.make_async_remote_copy(
            src_ref=src, dst_ref=dst, send_sem=send, recv_sem=recv,
            device_id={"ep": dev}, device_id_type=pl.DeviceIdType.MESH,
        )

    def many(ref, sem):
        return pltpu.make_async_copy(ref, ref, sem)

    def load_tokens(j):
        return pltpu.make_async_copy(
            tokens.at[:, pl.ds(j * kc, kc)], rx.at[j, line + z], tok_sem.at[j]
        )

    def load_g(j):
        s = j % slots
        return pltpu.make_async_copy(wg.at[pl.ds(j * kc, kc), :], ring_g.at[s], g_sem.at[s])

    def load_u(j):
        s = j % slots
        return pltpu.make_async_copy(wu.at[pl.ds(j * kc, kc), :], ring_u.at[s], u_sem.at[s])

    def load_d(c):
        cols = pl.ds(*spans[c])
        return pltpu.make_async_copy(wd.at[:, cols], down.at[:, cols], d_sem.at[c])

    barrier = pltpu.get_barrier_semaphore()

    def greet(dev):
        pl.semaphore_signal(barrier, inc=1, device_id={"ep": dev}, device_id_type=pl.DeviceIdType.MESH)

    for i in range(1, chips):
        greet(lax.rem(chip + i, chips) * 2 + core)
    greet(peer)

    for j in range(units):
        load_tokens(j).start()
    for j in range(min(slots, units)):
        load_g(j).start(priority=1)
        load_u(j).start(priority=1)

    lane = lax.broadcasted_iota(jnp.int32, (rows, AUX), 1)
    name = jnp.where(lane < EXPERTS, lane, lane - EXPERTS)
    weight = jnp.zeros((rows, AUX), jnp.float32)
    for k in range(routes.shape[1]):
        weight = weight + jnp.where(routes[:, k : k + 1] == name, gates[:, k : k + 1], 0.0)
    high = weight.astype(jnp.bfloat16).astype(jnp.float32)
    ax[line + z] = jnp.where(
        lane < EXPERTS, high, jnp.where(lane < 2 * EXPERTS, weight - high, 0.0)
    ).astype(jnp.bfloat16)

    pl.semaphore_wait(barrier, chips)

    for j in range(units):
        load_tokens(j).wait()
        for i in range(1, outer):
            slot = rx.at[j, line + z]
            remote(slot, slot, tz_send.at[j], tz_recv.at[j], place(along_z(i), x)).start()
    for i in range(1, outer):
        slot = ax.at[line + z]
        remote(slot, slot, ax_send.at[0], ax_recv.at[0], place(along_z(i), x)).start()

    def hop_x(j):
        many(rx.at[j, pl.ds(0, outer - 1)], tz_recv.at[j]).wait()
        for i in range(1, inner):
            part = rx.at[j, pl.ds(line, outer)]
            remote(part, part, tx_send.at[j], tx_recv.at[j], place(z, along_x(i))).start()

    def relay(j):
        half = rx.at[j, pl.ds(core * chips, chips)]
        return remote(half, half, re_send.at[j], re_recv.at[j], peer)

    def hop_core(j):
        many(rx.at[j, pl.ds(0, chips - outer)], tx_recv.at[j]).wait()
        relay(j).start()

    half_ax = ax.at[pl.ds(core * chips, chips)]
    relay_aux = remote(half_ax, half_ax, ax_send.at[2], ax_recv.at[2], peer)

    lead = min(units, LEAD)
    ahead = min(units, LEAD2)
    for j in range(lead):
        hop_x(j)
    sent = 0
    for j in range(lead, units):
        hop_x(j)
        if sent < ahead:
            hop_core(sent)
            sent += 1
    many(ax.at[pl.ds(0, outer - 1)], ax_recv.at[0]).wait()
    for i in range(1, inner):
        part = ax.at[pl.ds(line, outer)]
        remote(part, part, ax_send.at[1], ax_recv.at[1], place(z, along_x(i))).start()

    group = max(1, 16 // rows)

    def gather_rows(j, b):
        parts = [rx[j, b * group + i].astype(jnp.float32) for i in range(group)]
        whole = parts[0] if group == 1 else jnp.concatenate(parts, axis=0)
        return whole.astype(jnp.bfloat16)

    issued, waited = 0, 0

    def feed(others, least=0):
        nonlocal issued
        while issued < outs and (
            issued < least
            or others + hidden * sum(n for _, n in spans[waited : issued + 1]) <= WINDOW * 2 * kc * hidden
        ):
            load_d(issued).start(priority=1)
            issued += 1

    feed(units * 2 * kc * hidden, AHEAD)
    for j in range(units):
        while sent < min(units, j + 1 + ahead):
            hop_core(sent)
            sent += 1
        relay(j).wait_recv()
        if devices // group <= 16:
            for b in range(devices // group):
                xb[b * group * rows : (b + 1) * group * rows, :] = gather_rows(j, b)
        else:
            @pl.loop(0, devices // group)
            def _(b):
                xb[pl.ds(pl.multiple_of(b * group * rows, group * rows), group * rows), :] = gather_rows(j, b)
        load_g(j).wait()
        load_u(j).wait()
        s = j % slots

        for n in range(hidden // tile):
            cols = pl.ds(n * tile, tile)
            pg = jnp.dot(xb[...], ring_g[s, :, cols], preferred_element_type=jnp.float32)
            pu = jnp.dot(xb[...], ring_u[s, :, cols], preferred_element_type=jnp.float32)
            if j == 0:
                acc_g[:, cols] = pg
                acc_u[:, cols] = pu
            elif j < units - 1:
                acc_g[:, cols] += pg
                acc_u[:, cols] += pu
            else:
                g = acc_g[:, cols] + pg
                u = acc_u[:, cols] + pu
                hid[:, cols] = (g / (1.0 + jnp.exp(-g)) * u).astype(jnp.bfloat16)

        if j + slots < units:
            load_g(j + slots).start(priority=1)
            load_u(j + slots).start(priority=1)
        feed(kc * 2 * hidden * max(0, min(units, j + 1 + slots) - j - 1))

    many(ax.at[pl.ds(0, chips - outer)], ax_recv.at[1]).wait()
    relay_aux.start()
    relay_aux.wait_recv()
    expert = me // (devices // EXPERTS)
    spot = lax.broadcasted_iota(jnp.int32, (group * rows, AUX), 1)
    hot = (spot == expert) | (spot == expert + EXPERTS)

    def share_rows(b):
        parts = [ax[b * group + i].astype(jnp.float32) for i in range(group)]
        whole = parts[0] if group == 1 else jnp.concatenate(parts, axis=0)
        total = jnp.sum(jnp.where(hot, whole, 0.0), axis=1, keepdims=True)
        return jnp.broadcast_to(total, (group * rows, AUX))

    if devices // group <= 16:
        for b in range(devices // group):
            share[b * group * rows : (b + 1) * group * rows, :] = share_rows(b)
    else:
        @pl.loop(0, devices // group)
        def _(b):
            share[pl.ds(pl.multiple_of(b * group * rows, group * rows), group * rows), :] = share_rows(b)

    def swap(c):
        cols = pl.ds(*spans[c])
        return remote(mine.at[other, :, cols], theirs.at[:, cols], ob_send.at[c], ob_recv.at[c], peer)

    def sum_core(c):
        cols = pl.ds(*spans[c])
        swap(c).wait_recv()
        for i in range(1, inner):
            to = along_x(i)
            at = pl.ds(pl.multiple_of(to * block, block), block)
            xs[to, :, cols] = (mine[core, at, cols] + theirs[at, cols]).astype(jnp.bfloat16)
            remote(
                xs.at[to, :, cols], xr.at[x, :, cols], rx_send.at[c], rx_recv.at[c], place(z, to)
            ).start()
        at = pl.ds(pl.multiple_of(x * block, block), block)
        own[:, cols] = mine[core, at, cols] + theirs[at, cols]

    def sum_x(c):
        cols = pl.ds(*spans[c])
        many(xr.at[pl.ds(0, inner - 1), :, cols], rx_recv.at[c]).wait()
        total = own[:, cols]
        for i in range(1, inner):
            total = total + xr[along_x(i), :, cols].astype(jnp.float32)
        for b in range(outer):
            zs[b, :, cols] = total[b * rows : (b + 1) * rows].astype(jnp.bfloat16)
        for i in range(1, outer):
            to = along_z(i)
            remote(
                zs.at[to, :, cols], zr.at[z, :, cols], rz_send.at[c], rz_recv.at[c], place(to, x)
            ).start()
        zr[z, :, cols] = zs[z, :, cols]

    def sum_z(c):
        cols = pl.ds(*spans[c])
        many(zr.at[pl.ds(0, outer - 1), :, cols], rz_recv.at[c]).wait()
        total = zr[0, :, cols].astype(jnp.float32)
        for b in range(1, outer):
            total = total + zr[b, :, cols].astype(jnp.float32)
        out[:, cols] = total.astype(jnp.bfloat16)

    near = spans[outs - DIRECT][0]

    def give(c):
        at, size = spans[c]
        cols, mine_at = pl.ds(at, size), pl.ds(at - near, size)
        swap(c).wait_recv()
        both = mine[core, :, cols] + theirs[:, cols]
        for b in range(chips):
            ds[b % outer * inner + b // outer, :, mine_at] = both[b * rows : (b + 1) * rows].astype(jnp.bfloat16)
        for i in range(1, chips):
            to = lax.rem(chip + i, chips)
            remote(
                ds.at[to, :, mine_at], dr.at[chip, :, mine_at], rz_send.at[c], rz_recv.at[c], to * 2 + core
            ).start()
        dr[chip, :, mine_at] = ds[chip, :, mine_at]

    def sum_all(c):
        at, size = spans[c]
        cols, mine_at = pl.ds(at, size), pl.ds(at - near, size)
        many(dr.at[pl.ds(0, chips - 1), :, mine_at], rz_recv.at[c]).wait()
        total = dr[0, :, mine_at].astype(jnp.float32)
        for b in range(1, chips):
            total = total + dr[b, :, mine_at].astype(jnp.float32)
        out[:, cols] = total.astype(jnp.bfloat16)

    def stage_1(c):
        if c < outs - DIRECT:
            sum_core(c)
        else:
            give(c)

    def stage_2(c):
        if c < outs - DIRECT:
            sum_x(c)

    def stage_3(c):
        if c < outs - DIRECT:
            sum_z(c)
        else:
            sum_all(c)

    stages = ((LAGS[0], stage_1), (LAGS[1], stage_2), (LAGS[2], stage_3))
    for c in range(outs + LAGS[2]):
        if c < outs:
            load_d(c).wait()
            waited += 1
            feed(0)
            at, size = spans[c]
            sub = min(tile, size)
            for n in range(size // sub):
                cols = pl.ds(at + n * sub, sub)
                o = jnp.dot(hid[...], down[:, cols], preferred_element_type=jnp.float32)
                o = o * share[:, :1]
                mine[0, :, cols] = o[:mates]
                mine[1, :, cols] = o[mates:]
            swap(c).start()
        for lag, stage in stages:
            if 0 <= c - lag < outs:
                stage(c - lag)

    for j in range(units):
        many(rx.at[j, pl.ds(0, outer - 1)], tz_send.at[j]).wait()
        many(rx.at[j, pl.ds(0, chips - outer)], tx_send.at[j]).wait()
        relay(j).wait_send()
    many(ax.at[pl.ds(0, outer - 1)], ax_send.at[0]).wait()
    many(ax.at[pl.ds(0, chips - outer)], ax_send.at[1]).wait()
    relay_aux.wait_send()
    for c in range(outs):
        cols = pl.ds(*spans[c])
        swap(c).wait_send()
        if c < outs - DIRECT:
            many(xr.at[pl.ds(0, inner - 1), :, cols], rx_send.at[c]).wait()
            many(zr.at[pl.ds(0, outer - 1), :, cols], rz_send.at[c]).wait()
        else:
            cols = pl.ds(spans[c][0] - near, spans[c][1])
            many(dr.at[pl.ds(0, chips - 1), :, cols], rz_send.at[c]).wait()


def layer(tokens, routes, gates, wg, wu, wd):
    devices = lax.axis_size("ep")
    rows, width = tokens.shape
    hidden = wg.shape[1]
    chips = devices // 2
    inner = split_chips(chips)
    outer = chips // inner
    kc = piece(width, 512)
    tile = piece(hidden, 512)
    spans = column_spans(width, 1024)
    near = spans[len(spans) - DIRECT][0]
    units, outs = width // kc, len(spans)
    slots = min(SLOTS, units)
    batch = devices * rows
    bf16, f32 = jnp.bfloat16, jnp.float32
    dma = pltpu.SemaphoreType.DMA
    anywhere = pl.BlockSpec(memory_space=pl.ANY)
    vmem = pl.BlockSpec(memory_space=pltpu.VMEM)
    return pl.pallas_call(
        functools.partial(kernel, devices, inner, kc, spans, tile),
        out_shape=pltpu.VMEM((rows, width), bf16),
        in_specs=[anywhere, vmem, vmem, anywhere, anywhere, anywhere],
        out_specs=vmem,
        scratch_shapes=[
            pltpu.VMEM((slots, kc, hidden), bf16),
            pltpu.VMEM((slots, kc, hidden), bf16),
            pltpu.VMEM((hidden, width), bf16),
            pltpu.VMEM((units, devices, rows, kc), bf16),
            pltpu.VMEM((devices, rows, AUX), bf16),
            pltpu.VMEM((batch, kc), bf16),
            pltpu.VMEM((batch, hidden), f32),
            pltpu.VMEM((batch, hidden), f32),
            pltpu.VMEM((batch, hidden), bf16),
            pltpu.VMEM((batch, AUX), f32),
            pltpu.VMEM((2, chips * rows, width), f32),
            pltpu.VMEM((chips * rows, width), f32),
            pltpu.VMEM((outer * rows, near), f32),
            pltpu.VMEM((inner, outer * rows, near), bf16),
            pltpu.VMEM((inner, outer * rows, near), bf16),
            pltpu.VMEM((outer, rows, near), bf16),
            pltpu.VMEM((outer, rows, near), bf16),
            pltpu.VMEM((chips, rows, width - near), bf16),
            pltpu.VMEM((chips, rows, width - near), bf16),
            dma((units,)), dma((slots,)), dma((slots,)), dma((outs,)),
            dma((units,)), dma((units,)), dma((units,)), dma((units,)), dma((units,)), dma((units,)),
            dma((outs,)), dma((outs,)), dma((outs,)), dma((outs,)), dma((outs,)), dma((outs,)),
            dma((3,)), dma((3,)),
        ],
        compiler_params=pltpu.CompilerParams(
            collective_id=0, has_side_effects=True, vmem_limit_bytes=66_800_000
        ),
    )(tokens, routes, gates, wg, wu, wd)


def solution(mesh):
    placed = (
        P(("groups", "ep"), None),
        P(("groups", "ep"), None),
        P(("groups", "ep"), None),
        P(None, "ep"),
        P(None, "ep"),
        P("ep", None),
    )
    return jax.shard_map(
        layer, mesh=mesh, in_specs=placed, out_specs=P(("groups", "ep"), None), check_vma=False
    )
```
